32 devices in a mesh: gx: 4 (over z), gy: 4 (over y, x), gz: 2 (over core).
Axes of the slice: x: 2, y: 2, z: 4, core: 2. Of those that a mesh axis runs over, the one named last changes fastest.
Arguments:
- schur: bfloat16 [4, 4, 2, 2048, 2048], P('gx', 'gy', 'gz'), may hold values from -0.09375 to 0.09375
- interface_diag: float32 [4, 4, 2, 2048], P('gx', 'gy', 'gz'), may hold values from 2 to 4
- precond: float32 [4, 4, 2, 16, 128, 128], P('gx', 'gy', 'gz'), may hold values from -0.3 to 0.8
- load: bfloat16 [4, 4, 2, 2048, 256], P('gx', 'gy', 'gz'), may hold values from -170 to 170
- face_blocks: int32 [4, 4, 2, 6, 2], P('gx', 'gy', 'gz'), may hold values from 0 to 16, as said below
Outputs:
- solution: float32 [4, 4, 2, 2048, 256], P('gx', 'gy', 'gz')
- residual_norm: float32 [256], replicated
The draws below stay inside these ranges and needn't reach their ends.
Inputs may be any that keep to these rules, and one draw needn't show every extreme that they name: `face_blocks`: for each subdomain p and direction d (0, 1: next and previous along the first grid dimension; 2, 3 and 4, 5 likewise along the second and third), slots 0 to n - 1 hold block numbers below 16 shared with the neighbour in that direction, where n (1 to 2 inside the grid, 0 across its boundary) equals the neighbour's n for the opposite direction, and the neighbour's slot k of the opposite direction holds the block that shares with p's slot k; the remaining slots hold 16; no block number appears twice in one subdomain's table; some face shares 2 blocks in every draw.
All inputs are finite; a program needn't handle non-finite values.
Results may differ from the reference program's by a relative error of at most 0.0008.
Values sent between devices are 32-bit elements; how exact they have to be, the bound alone decides.
A program may use at most 128 MiB of HBM per device.

```python
import math
import jax
import jax.numpy as jnp
from jax import lax

BLK = 128
NBLK = 16
IFACE = 2048
CAP = 2
NRHS = 256
SUB_X = 4
SUB_Y = 4
SUB_Z = 2


def draw_precond(key, part):
    full_shape = (SUB_X, SUB_Y, SUB_Z, NBLK, BLK, BLK)
    key_diag, key_off = jax.random.split(jax.random.fold_in(key, 11))
    diagonal = 1.0 / jax.random.uniform(key_diag, full_shape[:-1], jnp.float32, 2.0, 4.0)
    coupling = jnp.clip(jax.random.normal(key_off, full_shape, jnp.float32), -6.0, 6.0) * (0.12 / math.sqrt(BLK))
    identity = jnp.eye(BLK, dtype=jnp.float32)
    return coupling + diagonal[..., None] * identity


def ramp_factor(length):
    return jnp.power(3.0, jnp.arange(length, dtype=jnp.float32) / max(length - 1, 1))


def draw_load(key, part):
    key_base = jax.random.fold_in(jax.random.fold_in(key, 5), 0)
    key_rows = jax.random.fold_in(jax.random.fold_in(key, 5), 2)
    key_cols = jax.random.fold_in(jax.random.fold_in(key, 5), 3)
    full_shape = (SUB_X, SUB_Y, SUB_Z, NBLK * BLK, NRHS)
    row_scale = jnp.exp(jax.random.uniform(key_rows, full_shape[:4] + (1,), jnp.float32, 0.0, math.log(10.0)))
    col_scale = jnp.exp(jax.random.uniform(key_cols, (NRHS,), jnp.float32, 0.0, math.log(10.0)))
    position = ramp_factor(SUB_X)[:, None, None] * ramp_factor(SUB_Y)[None, :, None] * ramp_factor(SUB_Z)[None, None, :]
    base = jnp.clip(jax.random.normal(key_base, full_shape, jnp.float32), -6.0, 6.0)
    values = 0.01 * base * row_scale * col_scale * position[..., None, None]
    return values.astype(jnp.bfloat16)


def pair_counts(pair_key, axis_id):
    grid_shape = [SUB_X, SUB_Y, SUB_Z]
    grid_shape[axis_id] = grid_shape[axis_id] - 1
    counts = jax.random.randint(pair_key, tuple(grid_shape), 1, CAP + 1, dtype=jnp.int32)
    if grid_shape[axis_id] > 0:
        counts = counts.at[0, 0, 0].set(CAP)
    pad_upper = [(0, 0)] * 3
    pad_upper[axis_id] = (0, 1)
    pad_lower = [(0, 0)] * 3
    pad_lower[axis_id] = (1, 0)
    return (jnp.pad(counts, pad_upper), jnp.pad(counts, pad_lower))


def draw_face_blocks(key, part):
    key_x, key_y, key_z, key_perm = jax.random.split(jax.random.fold_in(key, 7), 4)
    upper_x, lower_x = pair_counts(key_x, 0)
    upper_y, lower_y = pair_counts(key_y, 1)
    upper_z, lower_z = pair_counts(key_z, 2)
    dir_counts = jnp.stack([upper_x, lower_x, upper_y, lower_y, upper_z, lower_z], axis=-1)
    offsets = jnp.cumsum(dir_counts, axis=-1) - dir_counts
    subdomains = SUB_X * SUB_Y * SUB_Z
    perm_keys = jax.random.split(key_perm, subdomains)
    orders = jax.vmap(lambda one_key: jax.random.permutation(one_key, NBLK))(perm_keys).astype(jnp.int32)
    orders = orders.reshape(SUB_X, SUB_Y, SUB_Z, 1, NBLK)
    slot_ids = jnp.arange(CAP, dtype=jnp.int32)
    positions = jnp.minimum(offsets[..., None] + slot_ids, NBLK - 1).astype(jnp.int32)
    picked = jnp.take_along_axis(orders, positions.reshape(SUB_X, SUB_Y, SUB_Z, 1, 6 * CAP), axis=-1)
    picked = picked.reshape(SUB_X, SUB_Y, SUB_Z, 6, CAP)
    valid = slot_ids < dir_counts[..., None]
    return jnp.where(valid, picked, NBLK).astype(jnp.int32)


def block_levels(own_key, shape, pieces, least, top_value):
    gain = 1.0
    for dim, parts in pieces:
        draws = jax.random.uniform(jax.random.fold_in(jax.random.fold_in(own_key, 6), dim), (parts,), jnp.float32, least / len(pieces), top_value / len(pieces))
        gain = gain * jnp.repeat(jnp.exp(draws), shape[dim] // parts).reshape((-1,) + (1,) * (len(shape) - 1 - dim))
    return gain


def gaussian(stream_key, shape, width, reach, shards=(), kind=jnp.bfloat16):
    result = width * jax.random.normal(stream_key, shape, jnp.float32)
    if shards:
        result = result * block_levels(stream_key, shape, shards, -0.22, 0.18)
    return jnp.clip(result, -reach, reach).astype(kind)


def setup_inputs(seed: int = 0) -> dict:
    seeds = jax.random.split(jax.random.key(seed), 6)
    return {
        "schur": gaussian(seeds[0], (SUB_X, SUB_Y, SUB_Z, IFACE, IFACE), (2 * IFACE) ** -0.5, 0.09375, ((0, 4), (1, 4), (2, 2))),
        "interface_diag": jnp.clip(jnp.exp(math.log(4.0) - 0.6931472 * jax.random.uniform(seeds[1], (SUB_X, SUB_Y, SUB_Z, IFACE), jnp.float32) ** block_levels(seeds[1], (SUB_X, SUB_Y, SUB_Z, IFACE), ((0, 4), (1, 4), (2, 2)), -0.2, 0.2)), 2.0, 4.0),
        "precond": draw_precond(jax.random.fold_in(seeds[5], 71), 0),
        "load": draw_load(jax.random.fold_in(seeds[5], 71), 0),
        "face_blocks": draw_face_blocks(jax.random.fold_in(seeds[5], 71), 0),
    }


epsilon = 1e-06

def find_live(face_blocks):
    slot_hits = face_blocks[..., None] == jnp.arange(NBLK, dtype=jnp.int32)
    return jnp.any(slot_hits, axis=(3, 4)).astype(jnp.float32)

def from_next(values, axis_id):
    length = values.shape[axis_id]
    pad_spec = [(0, 0)] * values.ndim
    pad_spec[axis_id] = (0, 1)
    return lax.slice_in_dim(jnp.pad(values, pad_spec), 1, length + 1, axis=axis_id)

def from_prev(values, axis_id):
    length = values.shape[axis_id]
    pad_spec = [(0, 0)] * values.ndim
    pad_spec[axis_id] = (1, 0)
    return lax.slice_in_dim(jnp.pad(values, pad_spec), 0, length, axis=axis_id)

def assemble(blocks, face_blocks, live_mask):
    grid_shape = blocks.shape[:3]
    row_width = blocks.shape[-1]
    subdomains = grid_shape[0] * grid_shape[1] * grid_shape[2]
    flattened = blocks.reshape(subdomains, NBLK, BLK, row_width)
    extended = jnp.concatenate([flattened, jnp.zeros((subdomains, 1, BLK, row_width), jnp.float32)], axis=1)
    slot_index = face_blocks.reshape(subdomains, 6 * CAP).astype(jnp.int32)
    packed = jax.vmap(lambda table, picks: table[picks])(extended, slot_index)
    packed = packed.reshape(grid_shape + (6, CAP, BLK, row_width))
    arrived = jnp.stack([from_next(packed[:, :, :, 1], 0), from_prev(packed[:, :, :, 0], 0), from_next(packed[:, :, :, 3], 1), from_prev(packed[:, :, :, 2], 1), from_next(packed[:, :, :, 5], 2), from_prev(packed[:, :, :, 4], 2)], axis=3)
    arrived = arrived.reshape(subdomains, 6 * CAP, BLK, row_width)
    extended = jax.vmap(lambda table, picks, extra: table.at[picks].add(extra))(extended, slot_index, arrived)
    return extended[:, :NBLK].reshape(blocks.shape) * live_mask[..., None, None]

def inner_product(left_vec, right_vec):
    return 0.5 * lax.optimization_barrier(jnp.sum(left_vec * right_vec, axis=(0, 1, 2, 3, 4)))

def precondition(vector, precond, face_blocks, live_mask):
    partial_value = jnp.einsum('xyzbij,xyzbjr->xyzbir', precond, vector, precision=lax.Precision.HIGHEST)
    return assemble(partial_value, face_blocks, live_mask)

def operate(vector, schur, interface_diag, face_blocks, live_mask):
    subdomains = SUB_X * SUB_Y * SUB_Z
    flat_schur = schur.reshape(subdomains, IFACE, IFACE)
    flat_vector = vector.reshape(subdomains, IFACE, NRHS)
    product = lax.map(lambda pair: jnp.dot(pair[0], pair[1].astype(jnp.bfloat16), preferred_element_type=jnp.float32), (flat_schur, flat_vector))
    partial_value = product + interface_diag.reshape(subdomains, IFACE, 1) * flat_vector
    return assemble(partial_value.reshape(vector.shape), face_blocks, live_mask)

def reference(schur, interface_diag, precond, load, face_blocks):
    live_mask = find_live(face_blocks)
    block_shape = (SUB_X, SUB_Y, SUB_Z, NBLK, BLK, NRHS)
    assembled_load = assemble(load.astype(jnp.float32).reshape(block_shape), face_blocks, live_mask)
    initial = jnp.sqrt(inner_product(assembled_load, assembled_load) + epsilon)
    basis_first = assembled_load / initial
    precond_first = precondition(basis_first, precond, face_blocks, live_mask)
    working = operate(precond_first, schur, interface_diag, face_blocks, live_mask)
    diag_first = inner_product(working, basis_first)
    working = working - diag_first * basis_first
    below_first = jnp.sqrt(inner_product(working, working) + epsilon)
    basis_second = working / below_first
    precond_second = precondition(basis_second, precond, face_blocks, live_mask)
    working = operate(precond_second, schur, interface_diag, face_blocks, live_mask)
    upper_second = inner_product(working, basis_first)
    working = working - upper_second * basis_first
    diag_second = inner_product(working, basis_second)
    working = working - diag_second * basis_second
    below_second = jnp.sqrt(inner_product(working, working) + epsilon)
    radius_first = jnp.sqrt(diag_first * diag_first + below_first * below_first)
    cosine_first = diag_first / radius_first
    sine_first = below_first / radius_first
    rotated_top = cosine_first * upper_second + sine_first * diag_second
    rotated_low = cosine_first * diag_second - sine_first * upper_second
    radius_second = jnp.sqrt(rotated_low * rotated_low + below_second * below_second)
    cosine_second = rotated_low / radius_second
    sine_second = below_second / radius_second
    weight_second = -initial * sine_first * cosine_second / radius_second
    weight_first = (initial * cosine_first - rotated_top * weight_second) / radius_first
    solution = weight_first * precond_first + weight_second * precond_second
    residual_norm = initial * sine_first * sine_second
    return (solution.reshape(SUB_X, SUB_Y, SUB_Z, IFACE, NRHS), residual_norm)
```

```python
import functools

import jax
import jax.numpy as jnp
from jax import lax
from jax.experimental import pallas as pl
from jax.experimental.pallas import tpu as pltpu
from jax.sharding import PartitionSpec as P

EPS = 1e-06
MESH = pl.DeviceIdType.MESH
AXES = ("gx", "gy", "gz")
LANES = 128
F32 = jnp.float32
BF16 = jnp.bfloat16


def kernel(
    sizes,
    load_send,
    prec_send,
    schur_slots,
    diag_slots,
    mask_ref,
    out_ref,
    norm_ref,
    load_recv,
    prec_recv,
    prec_split,
    rhs,
    z1_ref,
    z2_ref,
    z_narrow,
    u1_send,
    u1_recv,
    q_ref,
    u2_send,
    u2_recv,
    plane_buf,
    line_buf,
    face_send,
    face_recv,
    plane_send,
    plane_recv,
    line_send,
    line_recv,
):
    nx, ny, nz = sizes
    planes = ny * nz
    cap, blk = prec_send.shape[1:3]
    cols = load_send.shape[-1]
    slots = 6 * cap
    rows = cap * blk
    gx, gy, gz = (lax.axis_index(a) for a in AXES)
    here = gy * nz + gz

    def plane_peer(step):
        other = lax.rem(here + step, planes)
        return (gx, other // nz, lax.rem(other, nz))

    def line_peer(step):
        return (lax.rem(gx + step, nx), gy, gz)

    barrier = pltpu.get_barrier_semaphore()
    for step in range(1, planes):
        pl.semaphore_signal(barrier, inc=1, device_id=plane_peer(step), device_id_type=MESH)
    for step in range(1, nx):
        pl.semaphore_signal(barrier, inc=1, device_id=line_peer(step), device_id_type=MESH)

    target, has = [], []
    for d in range(6):
        at = [gx, gy, gz]
        if d % 2 == 0:
            has.append(at[d // 2] + 1 < sizes[d // 2])
            at[d // 2] = at[d // 2] + 1
        else:
            has.append(at[d // 2] > 0)
            at[d // 2] = at[d // 2] - 1
        target.append(tuple(at))

    def face_copy(number, source, landing, d, slot):
        return pltpu.make_async_remote_copy(
            src_ref=source,
            dst_ref=landing.at[slot],
            send_sem=face_send.at[number, d],
            recv_sem=face_recv.at[number, slot],
            device_id=target[d],
            device_id_type=MESH,
        )

    def send_face(number, source, landing, d):
        @pl.when(has[d])
        def _():
            face_copy(number, source, landing, d, d ^ 1).start()

    def wait_face(number, source, landing, d):
        @pl.when(has[d])
        def _():
            face_copy(number, source, landing, d, d).wait_recv()

    def wait_sent(number, source, landing, d):
        @pl.when(has[d])
        def _():
            face_copy(number, source, landing, d, d ^ 1).wait_send()

    def reduce_start(number, buf, count, me, peer, send, recv):
        for step in range(1, count):
            pltpu.make_async_remote_copy(
                src_ref=buf.at[number, me],
                dst_ref=buf.at[number, me],
                send_sem=send.at[number, step - 1],
                recv_sem=recv.at[number, step - 1],
                device_id=peer(step),
                device_id_type=MESH,
            ).start()

    def reduce_wait(number, buf, count, me, peer, send, recv, sent):
        for step in range(1, count):
            came = me if sent else lax.rem(me + count - step, count)
            copy = pltpu.make_async_remote_copy(
                src_ref=buf.at[number, me],
                dst_ref=buf.at[number, came],
                send_sem=send.at[number, step - 1],
                recv_sem=recv.at[number, step - 1],
                device_id=peer(step),
                device_id_type=MESH,
            )
            if sent:
                copy.wait_send()
            else:
                copy.wait_recv()

    plane_args = (plane_buf, planes, here, plane_peer, plane_send, plane_recv)
    line_args = (line_buf, nx, gx, line_peer, line_send, line_recv)

    def pack(values):
        parts = []
        for value in values:
            row = jnp.sum(value, axis=0, keepdims=True)
            for j in range(cols // LANES):
                parts.append(row[:, j * LANES : (j + 1) * LANES])
        spare = plane_buf.shape[2] - len(parts)
        if spare:
            parts.append(jnp.zeros((spare, LANES), F32))
        return jnp.concatenate(parts, axis=0)

    def unpack(total, i):
        n = cols // LANES
        return jnp.concatenate([total[i * n + j : i * n + j + 1] for j in range(n)], axis=1)

    def total_of(buf, number, count):
        total = buf[number, 0]
        for i in range(1, count):
            total = total + buf[number, i]
        return total

    def folded(x):
        return jnp.sum(x.reshape(x.shape[0] // 8, 8, cols), axis=0)

    for d in range(6):
        @pl.when(jnp.logical_not(has[d]))
        def _(d=d):
            load_recv[d] = jnp.zeros(load_recv.shape[1:], F32)
            prec_recv[d] = jnp.zeros(prec_recv.shape[1:], F32)
            u1_recv[d] = jnp.zeros(u1_recv.shape[1:], F32)
            u2_recv[d] = jnp.zeros(u2_recv.shape[1:], F32)

    order = (2, 3, 0, 1, 4, 5)
    pl.semaphore_wait(barrier, planes - 1 + nx - 1)
    for d in order:
        send_face(0, load_send.at[d], load_recv, d)
    for d in order:
        send_face(1, prec_send.at[d], prec_recv, d)

    square = jnp.zeros((8, cols), F32)
    for d in order:
        wait_face(0, load_send.at[d], load_recv, d)
        value = load_send[d] + load_recv[d]
        rhs[d] = value
        square = square + folded(value * value)

    def precondition(s, value, wide):
        high = value.astype(BF16)
        low = (value - high.astype(F32)).astype(BF16)
        both = prec_split[s]
        z = jnp.dot(both, jnp.concatenate([high, high], axis=0), preferred_element_type=F32)
        z = z + jnp.dot(both[:, :blk], low, preferred_element_type=F32)
        wide[s] = z
        z_narrow[s * blk : (s + 1) * blk] = z.astype(BF16)

    def operate(d, wide):
        product = jnp.dot(
            schur_slots[d * rows : (d + 1) * rows], z_narrow[...], preferred_element_type=F32
        )
        scale = diag_slots[d * rows : (d + 1) * rows]
        scale = jnp.concatenate([scale] * (cols // LANES), axis=1)
        return product + scale * wide[d * cap : (d + 1) * cap].reshape(rows, cols)

    for d in order:
        wait_face(1, prec_send.at[d], prec_recv, d)
        for k in range(cap):
            s = d * cap + k
            block = prec_send[d, k] + prec_recv[d, k]
            high = block.astype(BF16)
            low = (block - high.astype(F32)).astype(BF16)
            prec_split[s] = jnp.concatenate([high, low], axis=1)
            precondition(s, rhs[d, k * blk : (k + 1) * blk], z1_ref)
    cross = jnp.zeros((8, cols), F32)
    for d in order:
        value = operate(d, z1_ref)
        u1_send[d] = value
        cross = cross + folded(value * rhs[d])

    plane_buf[0, here] = pack((0.5 * square, cross))
    reduce_start(0, *plane_args)
    for d in (2, 3, 4, 5):
        send_face(2, u1_send.at[d], u1_recv, d)
    reduce_wait(0, *plane_args, False)
    line_buf[0, gx] = total_of(plane_buf, 0, planes)
    reduce_start(0, *line_args)
    for d in (0, 1):
        send_face(2, u1_send.at[d], u1_recv, d)
    reduce_wait(0, *line_args, False)
    total = total_of(line_buf, 0, nx)
    load_square = unpack(total, 0)
    beta_square = load_square + EPS
    beta = jnp.sqrt(beta_square)
    h11 = unpack(total, 1) / beta_square

    square = jnp.zeros((8, cols), F32)
    for d in (4, 5, 0, 1, 2, 3):
        wait_face(2, u1_send.at[d], u1_recv, d)
        for k in range(cap):
            s = d * cap + k
            part = slice(k * blk, (k + 1) * blk)
            w = (u1_send[d, part] + u1_recv[d, part]) * mask_ref[s, 0:1]
            value = w - h11 * rhs[d, part]
            q_ref[d, part] = value
            square = square + folded(value * value)
            precondition(s, value, z2_ref)
    first = jnp.zeros((8, cols), F32)
    second = jnp.zeros((8, cols), F32)
    half = rows // 2

    def part_sent(d):
        return u2_send.at[d, pl.ds(half if d % 2 == 0 else 0, half)]

    for d in order:
        value = operate(d, z2_ref)
        u2_send[d] = value
        first = first + folded(value * rhs[d])
        second = second + folded(value * q_ref[d])
    for d in order:
        send_face(3, part_sent(d), u2_recv, d)
    work = jnp.zeros((8, cols), F32)
    step_rows = min(half, blk)
    for d in (4, 5, 0, 1, 2, 3):
        wait_face(3, part_sent(d), u2_recv, d)
        begin = 0 if d % 2 == 0 else half
        for row in range(0, half, step_rows):
            s = d * cap + (begin + row) // blk
            w = u2_send[d, begin + row : begin + row + step_rows]
            w = (w + u2_recv[d, row : row + step_rows]) * mask_ref[s, 0:1]
            work = work + folded(w * w)

    plane_buf[1, here] = pack((0.5 * square, first, second, work))
    reduce_start(1, *plane_args)
    reduce_wait(1, *plane_args, False)
    line_buf[1, gx] = total_of(plane_buf, 1, planes)
    reduce_start(1, *line_args)
    reduce_wait(1, *line_args, False)
    total = total_of(line_buf, 1, nx)
    q_square = unpack(total, 0)
    inverse = 1.0 / beta
    h21 = jnp.sqrt(q_square * inverse * inverse + EPS)
    t = inverse / h21
    h12 = unpack(total, 1) * t * inverse
    a22 = unpack(total, 2) * t * t
    ww = unpack(total, 3) * t * t
    n1 = load_square * inverse * inverse
    n2 = q_square * t * t
    g12 = h11 * EPS * inverse * t
    h22 = a22 - h12 * g12
    left = (
        ww
        - h12 * h12 * (2.0 - n1)
        - h22 * (2.0 * a22 - h22 * n2)
        + 2.0 * h12 * h22 * g12
    )
    h32 = jnp.sqrt(jnp.maximum(left, 0.0) + EPS)
    r1 = jnp.sqrt(h11 * h11 + h21 * h21)
    c1 = h11 / r1
    s1 = h21 / r1
    top = c1 * h12 + s1 * h22
    low = c1 * h22 - s1 * h12
    r2 = jnp.sqrt(low * low + h32 * h32)
    c2 = low / r2
    s2 = h32 / r2
    y2 = -beta * s1 * c2 / r2
    y1 = (beta * c1 - top * y2) / r1
    norm_ref[...] = beta * s1 * s2
    weight1 = y1 * inverse
    weight2 = y2 * t
    for k in range(slots):
        out_ref[k] = weight1 * z1_ref[k] + weight2 * z2_ref[k]

    for d in range(6):
        wait_sent(0, load_send.at[d], load_recv, d)
        wait_sent(1, prec_send.at[d], prec_recv, d)
        wait_sent(2, u1_send.at[d], u1_recv, d)
        wait_sent(3, part_sent(d), u2_recv, d)
    for number in range(2):
        reduce_wait(number, *plane_args, True)
        reduce_wait(number, *line_args, True)


def gather(table, schur_hbm, diag_ref, precond, load, load_out, prec_out, schur_out, diag_out, mask_out, strips, sems):
    nblk, blk, _ = precond.shape
    cols = load.shape[-1]
    slots = table.shape[0]
    cap = slots // 6
    index = [jnp.minimum(table[s], nblk - 1) for s in range(slots)]
    copies = []
    for s in range(slots):
        at = pl.ds(pl.multiple_of(index[s] * blk, blk), blk)
        copies.append(pltpu.make_async_copy(schur_hbm.at[at], strips.at[s], sems.at[s]))
        copies[-1].start()
    eye = lax.broadcasted_iota(jnp.int32, (blk, blk), 0) == lax.broadcasted_iota(
        jnp.int32, (blk, blk), 1
    )
    for s in range(slots):
        d, k = divmod(s, cap)
        valid = table[s] < nblk
        load_out[d, k * blk : (k + 1) * blk] = jnp.where(valid, load[index[s]].astype(F32), 0.0)
        prec_out[d, k] = precond[index[s]]
        mask_out[s] = jnp.full((8, cols), jnp.where(valid, 1.0, 0.0), F32)
        line = diag_ref[:, pl.ds(pl.multiple_of(index[s] * blk, blk), blk)]
        column = jnp.sum(jnp.where(eye, line, 0.0), axis=1, keepdims=True)
        diag_out[s * blk : (s + 1) * blk] = jnp.broadcast_to(column, (blk, LANES))
    for s in range(slots):
        copies[s].wait()
        for t in range(slots):
            at = pl.ds(pl.multiple_of(index[t] * blk, blk), blk)
            schur_out[s * blk : (s + 1) * blk, t * blk : (t + 1) * blk] = strips[s, :, at]


def place(table, compact, out_ref):
    slots = table.shape[0]
    many = out_ref.shape[0]
    first = pl.program_id(0) * many
    for b in range(many):
        found = jnp.int32(slots)
        for s in range(slots):
            found = jnp.where(table[s] == first + b, jnp.int32(s), found)
        value = compact[jnp.minimum(found, slots - 1)]
        out_ref[b] = jnp.where(found < slots, value, 0.0)


def on_device(sizes, schur, interface_diag, precond, load, face_blocks):
    nblk, blk = precond.shape[3:5]
    cols = load.shape[-1]
    order = schur.shape[-1]
    cap = face_blocks.shape[-1]
    slots = 6 * cap
    rows = cap * blk
    nx, ny, nz = sizes
    planes = ny * nz
    packed = -(-(4 * cols // LANES) // 8) * 8
    vmem = pltpu.VMEM
    dma = pltpu.SemaphoreType.DMA
    anywhere = pl.BlockSpec(memory_space=pl.ANY)
    local = pl.BlockSpec(memory_space=pltpu.VMEM)
    scalars = pl.BlockSpec(memory_space=pltpu.SMEM)
    table = face_blocks.reshape(slots)
    mib = 1024 * 1024
    gathered = pl.pallas_call(
        gather,
        out_shape=(
            jax.ShapeDtypeStruct((6, rows, cols), F32),
            jax.ShapeDtypeStruct((6, cap, blk, blk), F32),
            jax.ShapeDtypeStruct((slots * blk, slots * blk), BF16),
            jax.ShapeDtypeStruct((slots * blk, LANES), F32),
            jax.ShapeDtypeStruct((slots, 8, cols), F32),
        ),
        in_specs=[scalars, anywhere, local, local, local],
        out_specs=(local,) * 5,
        scratch_shapes=[vmem((slots, blk, order), BF16), dma((slots,))],
        compiler_params=pltpu.CompilerParams(vmem_limit_bytes=24 * mib),
    )(
        table,
        schur.reshape(order, order),
        interface_diag.reshape(1, order),
        precond.reshape(nblk, blk, blk),
        load.reshape(nblk, blk, cols),
    )
    compact, norm = pl.pallas_call(
        functools.partial(kernel, sizes),
        out_shape=(
            jax.ShapeDtypeStruct((slots, blk, cols), F32),
            jax.ShapeDtypeStruct((1, cols), F32),
        ),
        in_specs=[local] * 5,
        out_specs=(local, local),
        scratch_shapes=[
            vmem((6, rows, cols), F32),
            vmem((6, cap, blk, blk), F32),
            vmem((slots, blk, 2 * blk), BF16),
            vmem((6, rows, cols), F32),
            vmem((slots, blk, cols), F32),
            vmem((slots, blk, cols), F32),
            vmem((slots * blk, cols), BF16),
            vmem((6, rows, cols), F32),
            vmem((6, rows, cols), F32),
            vmem((6, rows, cols), F32),
            vmem((6, rows, cols), F32),
            vmem((6, rows // 2, cols), F32),
            vmem((2, planes, packed, LANES), F32),
            vmem((2, nx, packed, LANES), F32),
            dma((4, 6)),
            dma((4, 6)),
            dma((2, max(planes - 1, 1))),
            dma((2, max(planes - 1, 1))),
            dma((2, max(nx - 1, 1))),
            dma((2, max(nx - 1, 1))),
        ],
        compiler_params=pltpu.CompilerParams(
            collective_id=0, has_side_effects=True, vmem_limit_bytes=32 * mib
        ),
    )(*gathered)
    many = 4 if nblk % 4 == 0 else 1
    result = pl.pallas_call(
        place,
        grid=(nblk // many,),
        out_shape=jax.ShapeDtypeStruct((nblk, blk, cols), F32),
        in_specs=[scalars, local],
        out_specs=pl.BlockSpec((many, blk, cols), lambda i: (i, 0, 0)),
        compiler_params=pltpu.CompilerParams(vmem_limit_bytes=16 * mib),
    )(table, compact)
    return result.reshape(1, 1, 1, nblk * blk, cols), norm.reshape(cols)


def solution(mesh):
    sizes = tuple(mesh.shape[a] for a in AXES)
    placed = (
        P("gx", "gy", "gz", None, None),
        P("gx", "gy", "gz", None),
        P("gx", "gy", "gz", None, None, None),
        P("gx", "gy", "gz", None, None),
        P("gx", "gy", "gz", None, None),
    )
    return jax.shard_map(
        functools.partial(on_device, sizes),
        mesh=mesh,
        in_specs=placed,
        out_specs=(P("gx", "gy", "gz", None, None), P()),
        check_vma=False,
    )
```

```python
import functools

import jax
import jax.numpy as jnp
from jax import lax
from jax.experimental import pallas as pl
from jax.experimental.pallas import tpu as pltpu
from jax.sharding import PartitionSpec as P

EPS = 1e-06
MESH = pl.DeviceIdType.MESH
AXES = ("gx", "gy", "gz")
LANES = 128
F32 = jnp.float32
BF16 = jnp.bfloat16


def kernel(
    sizes,
    load_send,
    prec_send,
    schur_slots,
    diag_slots,
    mask_ref,
    out_ref,
    norm_ref,
    load_recv,
    prec_recv,
    prec_split,
    rhs,
    z1_ref,
    z2_ref,
    z_narrow,
    u1_send,
    u1_recv,
    q_ref,
    u2_send,
    u2_recv,
    plane_buf,
    line_buf,
    face_send,
    face_recv,
    plane_send,
    plane_recv,
    line_send,
    line_recv,
):
    nx, ny, nz = sizes
    planes = ny * nz
    cap, blk = prec_send.shape[1:3]
    cols = load_send.shape[-1]
    slots = 6 * cap
    rows = cap * blk
    gx, gy, gz = (lax.axis_index(a) for a in AXES)
    here = gy * nz + gz

    def plane_peer(step):
        other = lax.rem(here + step, planes)
        return (gx, other // nz, lax.rem(other, nz))

    def line_peer(step):
        return (lax.rem(gx + step, nx), gy, gz)

    barrier = pltpu.get_barrier_semaphore()
    for step in range(1, planes):
        pl.semaphore_signal(barrier, inc=1, device_id=plane_peer(step), device_id_type=MESH)
    for step in range(1, nx):
        pl.semaphore_signal(barrier, inc=1, device_id=line_peer(step), device_id_type=MESH)

    target, has = [], []
    for d in range(6):
        at = [gx, gy, gz]
        if d % 2 == 0:
            has.append(at[d // 2] + 1 < sizes[d // 2])
            at[d // 2] = at[d // 2] + 1
        else:
            has.append(at[d // 2] > 0)
            at[d // 2] = at[d // 2] - 1
        target.append(tuple(at))

    def face_copy(number, source, landing, d, slot):
        return pltpu.make_async_remote_copy(
            src_ref=source,
            dst_ref=landing.at[slot],
            send_sem=face_send.at[number, d],
            recv_sem=face_recv.at[number, slot],
            device_id=target[d],
            device_id_type=MESH,
        )

    def send_face(number, source, landing, d):
        @pl.when(has[d])
        def _():
            face_copy(number, source, landing, d, d ^ 1).start()

    def wait_face(number, source, landing, d):
        @pl.when(has[d])
        def _():
            face_copy(number, source, landing, d, d).wait_recv()

    def wait_sent(number, source, landing, d):
        @pl.when(has[d])
        def _():
            face_copy(number, source, landing, d, d ^ 1).wait_send()

    def reduce_start(number, buf, count, me, peer, send, recv):
        for step in range(1, count):
            pltpu.make_async_remote_copy(
                src_ref=buf.at[number, me],
                dst_ref=buf.at[number, me],
                send_sem=send.at[number, step - 1],
                recv_sem=recv.at[number, step - 1],
                device_id=peer(step),
                device_id_type=MESH,
            ).start()

    def reduce_wait(number, buf, count, me, peer, send, recv, sent):
        for step in range(1, count):
            came = me if sent else lax.rem(me + count - step, count)
            copy = pltpu.make_async_remote_copy(
                src_ref=buf.at[number, me],
                dst_ref=buf.at[number, came],
                send_sem=send.at[number, step - 1],
                recv_sem=recv.at[number, step - 1],
                device_id=peer(step),
                device_id_type=MESH,
            )
            if sent:
                copy.wait_send()
            else:
                copy.wait_recv()

    plane_args = (plane_buf, planes, here, plane_peer, plane_send, plane_recv)
    line_args = (line_buf, nx, gx, line_peer, line_send, line_recv)

    def pack(values):
        parts = []
        for value in values:
            row = jnp.sum(value, axis=0, keepdims=True)
            for j in range(cols // LANES):
                parts.append(row[:, j * LANES : (j + 1) * LANES])
        spare = plane_buf.shape[2] - len(parts)
        if spare:
            parts.append(jnp.zeros((spare, LANES), F32))
        return jnp.concatenate(parts, axis=0)

    def unpack(total, i):
        n = cols // LANES
        return jnp.concatenate([total[i * n + j : i * n + j + 1] for j in range(n)], axis=1)

    def total_of(buf, number, count):
        total = buf[number, 0]
        for i in range(1, count):
            total = total + buf[number, i]
        return total

    def folded(x):
        return jnp.sum(x.reshape(x.shape[0] // 8, 8, cols), axis=0)

    for d in range(6):
        @pl.when(jnp.logical_not(has[d]))
        def _(d=d):
            load_recv[d] = jnp.zeros(load_recv.shape[1:], F32)
            prec_recv[d] = jnp.zeros(prec_recv.shape[1:], F32)
            u1_recv[d] = jnp.zeros(u1_recv.shape[1:], F32)
            u2_recv[d] = jnp.zeros(u2_recv.shape[1:], F32)

    order = (2, 3, 0, 1, 4, 5)
    pl.semaphore_wait(barrier, planes - 1 + nx - 1)
    for d in order:
        send_face(0, load_send.at[d], load_recv, d)
    for d in order:
        send_face(1, prec_send.at[d], prec_recv, d)

    square = jnp.zeros((8, cols), F32)
    for d in order:
        wait_face(0, load_send.at[d], load_recv, d)
        value = load_send[d] + load_recv[d]
        rhs[d] = value
        square = square + folded(value * value)

    def precondition(s, value, wide):
        high = value.astype(BF16)
        low = (value - high.astype(F32)).astype(BF16)
        both = prec_split[s]
        z = jnp.dot(both, jnp.concatenate([high, high], axis=0), preferred_element_type=F32)
        z = z + jnp.dot(both[:, :blk], low, preferred_element_type=F32)
        wide[s] = z
        z_narrow[s * blk : (s + 1) * blk] = z.astype(BF16)

    def operate(d, wide):
        product = jnp.dot(
            schur_slots[d * rows : (d + 1) * rows], z_narrow[...], preferred_element_type=F32
        )
        scale = diag_slots[d * rows : (d + 1) * rows]
        scale = jnp.concatenate([scale] * (cols // LANES), axis=1)
        return product + scale * wide[d * cap : (d + 1) * cap].reshape(rows, cols)

    for d in order:
        wait_face(1, prec_send.at[d], prec_recv, d)
        for k in range(cap):
            s = d * cap + k
            block = prec_send[d, k] + prec_recv[d, k]
            high = block.astype(BF16)
            low = (block - high.astype(F32)).astype(BF16)
            prec_split[s] = jnp.concatenate([high, low], axis=1)
            precondition(s, rhs[d, k * blk : (k + 1) * blk], z1_ref)
    cross = jnp.zeros((8, cols), F32)
    for d in order:
        value = operate(d, z1_ref)
        u1_send[d] = value
        cross = cross + folded(value * rhs[d])

    plane_buf[0, here] = pack((0.5 * square, cross))
    reduce_start(0, *plane_args)
    for d in (2, 3, 4, 5):
        send_face(2, u1_send.at[d], u1_recv, d)
    reduce_wait(0, *plane_args, False)
    line_buf[0, gx] = total_of(plane_buf, 0, planes)
    reduce_start(0, *line_args)
    for d in (0, 1):
        send_face(2, u1_send.at[d], u1_recv, d)
    reduce_wait(0, *line_args, False)
    total = total_of(line_buf, 0, nx)
    load_square = unpack(total, 0)
    beta_square = load_square + EPS
    beta = jnp.sqrt(beta_square)
    h11 = unpack(total, 1) / beta_square

    square = jnp.zeros((8, cols), F32)
    for d in (4, 5, 0, 1, 2, 3):
        wait_face(2, u1_send.at[d], u1_recv, d)
        for k in range(cap):
            s = d * cap + k
            part = slice(k * blk, (k + 1) * blk)
            w = (u1_send[d, part] + u1_recv[d, part]) * mask_ref[s, 0:1]
            value = w - h11 * rhs[d, part]
            q_ref[d, part] = value
            square = square + folded(value * value)
            precondition(s, value, z2_ref)
    first = jnp.zeros((8, cols), F32)
    second = jnp.zeros((8, cols), F32)
    half = rows // 2

    def part_sent(d):
        return u2_send.at[d, pl.ds(half if d % 2 == 0 else 0, half)]

    for i, d in enumerate(order):
        value = operate(d, z2_ref)
        u2_send[d] = value
        first = first + folded(value * rhs[d])
        second = second + folded(value * q_ref[d])
        if i:
            send_face(3, part_sent(order[i - 1]), u2_recv, order[i - 1])
    send_face(3, part_sent(order[-1]), u2_recv, order[-1])
    work = jnp.zeros((8, cols), F32)
    step_rows = min(half, blk)
    for d in (4, 5, 0, 1, 2, 3):
        wait_face(3, part_sent(d), u2_recv, d)
        begin = 0 if d % 2 == 0 else half
        for row in range(0, half, step_rows):
            s = d * cap + (begin + row) // blk
            w = u2_send[d, begin + row : begin + row + step_rows]
            w = (w + u2_recv[d, row : row + step_rows]) * mask_ref[s, 0:1]
            work = work + folded(w * w)

    plane_buf[1, here] = pack((0.5 * square, first, second, work))
    reduce_start(1, *plane_args)
    reduce_wait(1, *plane_args, False)
    line_buf[1, gx] = total_of(plane_buf, 1, planes)
    reduce_start(1, *line_args)
    reduce_wait(1, *line_args, False)
    total = total_of(line_buf, 1, nx)
    q_square = unpack(total, 0)
    inverse = 1.0 / beta
    h21 = jnp.sqrt(q_square * inverse * inverse + EPS)
    t = inverse / h21
    h12 = unpack(total, 1) * t * inverse
    a22 = unpack(total, 2) * t * t
    ww = unpack(total, 3) * t * t
    n1 = load_square * inverse * inverse
    n2 = q_square * t * t
    g12 = h11 * EPS * inverse * t
    h22 = a22 - h12 * g12
    left = (
        ww
        - h12 * h12 * (2.0 - n1)
        - h22 * (2.0 * a22 - h22 * n2)
        + 2.0 * h12 * h22 * g12
    )
    h32 = jnp.sqrt(jnp.maximum(left, 0.0) + EPS)
    r1 = jnp.sqrt(h11 * h11 + h21 * h21)
    c1 = h11 / r1
    s1 = h21 / r1
    top = c1 * h12 + s1 * h22
    low = c1 * h22 - s1 * h12
    r2 = jnp.sqrt(low * low + h32 * h32)
    c2 = low / r2
    s2 = h32 / r2
    y2 = -beta * s1 * c2 / r2
    y1 = (beta * c1 - top * y2) / r1
    norm_ref[...] = beta * s1 * s2
    weight1 = y1 * inverse
    weight2 = y2 * t
    for k in range(slots):
        out_ref[k] = weight1 * z1_ref[k] + weight2 * z2_ref[k]

    for d in range(6):
        wait_sent(0, load_send.at[d], load_recv, d)
        wait_sent(1, prec_send.at[d], prec_recv, d)
        wait_sent(2, u1_send.at[d], u1_recv, d)
        wait_sent(3, part_sent(d), u2_recv, d)
    for number in range(2):
        reduce_wait(number, *plane_args, True)
        reduce_wait(number, *line_args, True)


def gather(table, schur_hbm, diag_ref, precond, load, load_out, prec_out, schur_out, diag_out, mask_out, strips, sems):
    nblk, blk, _ = precond.shape
    cols = load.shape[-1]
    slots = table.shape[0]
    cap = slots // 6
    index = [jnp.minimum(table[s], nblk - 1) for s in range(slots)]
    copies = []
    for s in range(slots):
        at = pl.ds(pl.multiple_of(index[s] * blk, blk), blk)
        copies.append(pltpu.make_async_copy(schur_hbm.at[at], strips.at[s], sems.at[s]))
        copies[-1].start()
    eye = lax.broadcasted_iota(jnp.int32, (blk, blk), 0) == lax.broadcasted_iota(
        jnp.int32, (blk, blk), 1
    )
    for s in range(slots):
        d, k = divmod(s, cap)
        valid = table[s] < nblk
        load_out[d, k * blk : (k + 1) * blk] = jnp.where(valid, load[index[s]].astype(F32), 0.0)
        prec_out[d, k] = precond[index[s]]
        mask_out[s] = jnp.full((8, cols), jnp.where(valid, 1.0, 0.0), F32)
        line = diag_ref[:, pl.ds(pl.multiple_of(index[s] * blk, blk), blk)]
        column = jnp.sum(jnp.where(eye, line, 0.0), axis=1, keepdims=True)
        diag_out[s * blk : (s + 1) * blk] = jnp.broadcast_to(column, (blk, LANES))
    for s in range(slots):
        copies[s].wait()
        for t in range(slots):
            at = pl.ds(pl.multiple_of(index[t] * blk, blk), blk)
            schur_out[s * blk : (s + 1) * blk, t * blk : (t + 1) * blk] = strips[s, :, at]


def place(table, compact, out_ref):
    slots = table.shape[0]
    many = out_ref.shape[0]
    first = pl.program_id(0) * many
    for b in range(many):
        found = jnp.int32(slots)
        for s in range(slots):
            found = jnp.where(table[s] == first + b, jnp.int32(s), found)
        value = compact[jnp.minimum(found, slots - 1)]
        out_ref[b] = jnp.where(found < slots, value, 0.0)


def on_device(sizes, schur, interface_diag, precond, load, face_blocks):
    nblk, blk = precond.shape[3:5]
    cols = load.shape[-1]
    order = schur.shape[-1]
    cap = face_blocks.shape[-1]
    slots = 6 * cap
    rows = cap * blk
    nx, ny, nz = sizes
    planes = ny * nz
    packed = -(-(4 * cols // LANES) // 8) * 8
    vmem = pltpu.VMEM
    dma = pltpu.SemaphoreType.DMA
    anywhere = pl.BlockSpec(memory_space=pl.ANY)
    local = pl.BlockSpec(memory_space=pltpu.VMEM)
    scalars = pl.BlockSpec(memory_space=pltpu.SMEM)
    table = face_blocks.reshape(slots)
    mib = 1024 * 1024
    gathered = pl.pallas_call(
        gather,
        out_shape=(
            jax.ShapeDtypeStruct((6, rows, cols), F32),
            jax.ShapeDtypeStruct((6, cap, blk, blk), F32),
            jax.ShapeDtypeStruct((slots * blk, slots * blk), BF16),
            jax.ShapeDtypeStruct((slots * blk, LANES), F32),
            jax.ShapeDtypeStruct((slots, 8, cols), F32),
        ),
        in_specs=[scalars, anywhere, local, local, local],
        out_specs=(local,) * 5,
        scratch_shapes=[vmem((slots, blk, order), BF16), dma((slots,))],
        compiler_params=pltpu.CompilerParams(vmem_limit_bytes=24 * mib),
    )(
        table,
        schur.reshape(order, order),
        interface_diag.reshape(1, order),
        precond.reshape(nblk, blk, blk),
        load.reshape(nblk, blk, cols),
    )
    compact, norm = pl.pallas_call(
        functools.partial(kernel, sizes),
        out_shape=(
            jax.ShapeDtypeStruct((slots, blk, cols), F32),
            jax.ShapeDtypeStruct((1, cols), F32),
        ),
        in_specs=[local] * 5,
        out_specs=(local, local),
        scratch_shapes=[
            vmem((6, rows, cols), F32),
            vmem((6, cap, blk, blk), F32),
            vmem((slots, blk, 2 * blk), BF16),
            vmem((6, rows, cols), F32),
            vmem((slots, blk, cols), F32),
            vmem((slots, blk, cols), F32),
            vmem((slots * blk, cols), BF16),
            vmem((6, rows, cols), F32),
            vmem((6, rows, cols), F32),
            vmem((6, rows, cols), F32),
            vmem((6, rows, cols), F32),
            vmem((6, rows // 2, cols), F32),
            vmem((2, planes, packed, LANES), F32),
            vmem((2, nx, packed, LANES), F32),
            dma((4, 6)),
            dma((4, 6)),
            dma((2, max(planes - 1, 1))),
            dma((2, max(planes - 1, 1))),
            dma((2, max(nx - 1, 1))),
            dma((2, max(nx - 1, 1))),
        ],
        compiler_params=pltpu.CompilerParams(
            collective_id=0, has_side_effects=True, vmem_limit_bytes=32 * mib
        ),
    )(*gathered)
    many = 4 if nblk % 4 == 0 else 1
    result = pl.pallas_call(
        place,
        grid=(nblk // many,),
        out_shape=jax.ShapeDtypeStruct((nblk, blk, cols), F32),
        in_specs=[scalars, local],
        out_specs=pl.BlockSpec((many, blk, cols), lambda i: (i, 0, 0)),
        compiler_params=pltpu.CompilerParams(vmem_limit_bytes=16 * mib),
    )(table, compact)
    return result.reshape(1, 1, 1, nblk * blk, cols), norm.reshape(cols)


def solution(mesh):
    sizes = tuple(mesh.shape[a] for a in AXES)
    placed = (
        P("gx", "gy", "gz", None, None),
        P("gx", "gy", "gz", None),
        P("gx", "gy", "gz", None, None, None),
        P("gx", "gy", "gz", None, None),
        P("gx", "gy", "gz", None, None),
    )
    return jax.shard_map(
        functools.partial(on_device, sizes),
        mesh=mesh,
        in_specs=placed,
        out_specs=(P("gx", "gy", "gz", None, None), P()),
        check_vma=False,
    )
```

```python
import functools

import jax
import jax.numpy as jnp
from jax import lax
from jax.experimental import pallas as pl
from jax.experimental.pallas import tpu as pltpu
from jax.sharding import PartitionSpec as P

EPS = 1e-06
MESH = pl.DeviceIdType.MESH
AXES = ("gx", "gy", "gz")
LANES = 128
F32 = jnp.float32
BF16 = jnp.bfloat16


def kernel(
    sizes,
    load_send,
    prec_send,
    schur_slots,
    diag_slots,
    mask_ref,
    out_ref,
    norm_ref,
    load_recv,
    prec_recv,
    prec_split,
    rhs,
    z1_ref,
    z2_ref,
    z_narrow,
    u1_send,
    u1_recv,
    q_ref,
    u2_send,
    u2_recv,
    plane_buf,
    line_buf,
    face_send,
    face_recv,
    plane_send,
    plane_recv,
    line_send,
    line_recv,
):
    nx, ny, nz = sizes
    planes = ny * nz
    cap, blk = prec_send.shape[1:3]
    cols = load_send.shape[-1]
    slots = 6 * cap
    rows = cap * blk
    gx, gy, gz = (lax.axis_index(a) for a in AXES)
    here = gy * nz + gz

    def plane_peer(step):
        other = lax.rem(here + step, planes)
        return (gx, other // nz, lax.rem(other, nz))

    def line_peer(step):
        return (lax.rem(gx + step, nx), gy, gz)

    barrier = pltpu.get_barrier_semaphore()
    for step in range(1, planes):
        pl.semaphore_signal(barrier, inc=1, device_id=plane_peer(step), device_id_type=MESH)
    for step in range(1, nx):
        pl.semaphore_signal(barrier, inc=1, device_id=line_peer(step), device_id_type=MESH)

    target, has = [], []
    for d in range(6):
        at = [gx, gy, gz]
        if d % 2 == 0:
            has.append(at[d // 2] + 1 < sizes[d // 2])
            at[d // 2] = at[d // 2] + 1
        else:
            has.append(at[d // 2] > 0)
            at[d // 2] = at[d // 2] - 1
        target.append(tuple(at))

    def face_copy(number, source, landing, d, slot):
        return pltpu.make_async_remote_copy(
            src_ref=source,
            dst_ref=landing.at[slot],
            send_sem=face_send.at[number, d],
            recv_sem=face_recv.at[number, slot],
            device_id=target[d],
            device_id_type=MESH,
        )

    def send_face(number, source, landing, d):
        @pl.when(has[d])
        def _():
            face_copy(number, source, landing, d, d ^ 1).start()

    def wait_face(number, source, landing, d):
        @pl.when(has[d])
        def _():
            face_copy(number, source, landing, d, d).wait_recv()

    def wait_sent(number, source, landing, d):
        @pl.when(has[d])
        def _():
            face_copy(number, source, landing, d, d ^ 1).wait_send()

    def reduce_start(number, buf, count, me, peer, send, recv):
        for step in range(1, count):
            pltpu.make_async_remote_copy(
                src_ref=buf.at[number, me],
                dst_ref=buf.at[number, me],
                send_sem=send.at[number, step - 1],
                recv_sem=recv.at[number, step - 1],
                device_id=peer(step),
                device_id_type=MESH,
            ).start()

    def reduce_wait(number, buf, count, me, peer, send, recv, sent):
        for step in range(1, count):
            came = me if sent else lax.rem(me + count - step, count)
            copy = pltpu.make_async_remote_copy(
                src_ref=buf.at[number, me],
                dst_ref=buf.at[number, came],
                send_sem=send.at[number, step - 1],
                recv_sem=recv.at[number, step - 1],
                device_id=peer(step),
                device_id_type=MESH,
            )
            if sent:
                copy.wait_send()
            else:
                copy.wait_recv()

    plane_args = (plane_buf, planes, here, plane_peer, plane_send, plane_recv)
    line_args = (line_buf, nx, gx, line_peer, line_send, line_recv)

    def pack(values):
        parts = []
        for value in values:
            row = jnp.sum(value, axis=0, keepdims=True)
            for j in range(cols // LANES):
                parts.append(row[:, j * LANES : (j + 1) * LANES])
        spare = plane_buf.shape[2] - len(parts)
        if spare:
            parts.append(jnp.zeros((spare, LANES), F32))
        return jnp.concatenate(parts, axis=0)

    def unpack(total, i):
        n = cols // LANES
        return jnp.concatenate([total[i * n + j : i * n + j + 1] for j in range(n)], axis=1)

    def total_of(buf, number, count):
        total = buf[number, 0]
        for i in range(1, count):
            total = total + buf[number, i]
        return total

    def folded(x):
        return jnp.sum(x.reshape(x.shape[0] // 8, 8, cols), axis=0)

    for d in range(6):
        @pl.when(jnp.logical_not(has[d]))
        def _(d=d):
            load_recv[d] = jnp.zeros(load_recv.shape[1:], F32)
            prec_recv[d] = jnp.zeros(prec_recv.shape[1:], F32)
            u1_recv[d] = jnp.zeros(u1_recv.shape[1:], F32)
            u2_recv[d] = jnp.zeros(u2_recv.shape[1:], F32)

    order = (2, 3, 0, 1, 4, 5)
    arrival = (4, 5, 0, 1, 2, 3)
    pl.semaphore_wait(barrier, planes - 1 + nx - 1)
    for d in order:
        send_face(0, load_send.at[d], load_recv, d)
    for d in order:
        send_face(1, prec_send.at[d], prec_recv, d)

    square = jnp.zeros((8, cols), F32)
    for d in arrival:
        wait_face(0, load_send.at[d], load_recv, d)
        value = load_send[d] + load_recv[d]
        rhs[d] = value
        square = square + folded(value * value)

    def precondition(s, value, wide):
        high = value.astype(BF16)
        low = (value - high.astype(F32)).astype(BF16)
        both = prec_split[s]
        z = jnp.dot(both, jnp.concatenate([high, high], axis=0), preferred_element_type=F32)
        z = z + jnp.dot(both[:, :blk], low, preferred_element_type=F32)
        wide[s] = z
        z_narrow[s * blk : (s + 1) * blk] = z.astype(BF16)

    def operate(d, wide):
        product = jnp.dot(
            schur_slots[d * rows : (d + 1) * rows], z_narrow[...], preferred_element_type=F32
        )
        scale = diag_slots[d * rows : (d + 1) * rows]
        scale = jnp.concatenate([scale] * (cols // LANES), axis=1)
        return product + scale * wide[d * cap : (d + 1) * cap].reshape(rows, cols)

    for d in arrival:
        wait_face(1, prec_send.at[d], prec_recv, d)
        for k in range(cap):
            s = d * cap + k
            block = prec_send[d, k] + prec_recv[d, k]
            high = block.astype(BF16)
            low = (block - high.astype(F32)).astype(BF16)
            prec_split[s] = jnp.concatenate([high, low], axis=1)
            precondition(s, rhs[d, k * blk : (k + 1) * blk], z1_ref)
    cross = jnp.zeros((8, cols), F32)
    for d in order:
        value = operate(d, z1_ref)
        u1_send[d] = value
        cross = cross + folded(value * rhs[d])

    plane_buf[0, here] = pack((0.5 * square, cross))
    reduce_start(0, *plane_args)
    for d in (2, 3, 4, 5):
        send_face(2, u1_send.at[d], u1_recv, d)
    reduce_wait(0, *plane_args, False)
    line_buf[0, gx] = total_of(plane_buf, 0, planes)
    reduce_start(0, *line_args)
    for d in (0, 1):
        send_face(2, u1_send.at[d], u1_recv, d)
    reduce_wait(0, *line_args, False)
    total = total_of(line_buf, 0, nx)
    load_square = unpack(total, 0)
    beta_square = load_square + EPS
    beta = jnp.sqrt(beta_square)
    h11 = unpack(total, 1) / beta_square

    square = jnp.zeros((8, cols), F32)
    for d in arrival:
        wait_face(2, u1_send.at[d], u1_recv, d)
        for k in range(cap):
            s = d * cap + k
            part = slice(k * blk, (k + 1) * blk)
            w = (u1_send[d, part] + u1_recv[d, part]) * mask_ref[s, 0:1]
            value = w - h11 * rhs[d, part]
            q_ref[d, part] = value
            square = square + folded(value * value)
            precondition(s, value, z2_ref)
    first = jnp.zeros((8, cols), F32)
    second = jnp.zeros((8, cols), F32)
    half = rows // 2

    def part_sent(d):
        return u2_send.at[d, pl.ds(half if d % 2 == 0 else 0, half)]

    for i, d in enumerate(order):
        value = operate(d, z2_ref)
        u2_send[d] = value
        first = first + folded(value * rhs[d])
        second = second + folded(value * q_ref[d])
        if i:
            send_face(3, part_sent(order[i - 1]), u2_recv, order[i - 1])
    send_face(3, part_sent(order[-1]), u2_recv, order[-1])
    work = jnp.zeros((8, cols), F32)
    step_rows = min(half, blk)
    for d in arrival:
        wait_face(3, part_sent(d), u2_recv, d)
        begin = 0 if d % 2 == 0 else half
        for row in range(0, half, step_rows):
            s = d * cap + (begin + row) // blk
            w = u2_send[d, begin + row : begin + row + step_rows]
            w = (w + u2_recv[d, row : row + step_rows]) * mask_ref[s, 0:1]
            work = work + folded(w * w)

    plane_buf[1, here] = pack((0.5 * square, first, second, work))
    reduce_start(1, *plane_args)
    reduce_wait(1, *plane_args, False)
    line_buf[1, gx] = total_of(plane_buf, 1, planes)
    reduce_start(1, *line_args)
    reduce_wait(1, *line_args, False)
    total = total_of(line_buf, 1, nx)
    q_square = unpack(total, 0)
    inverse = 1.0 / beta
    h21 = jnp.sqrt(q_square * inverse * inverse + EPS)
    t = inverse / h21
    h12 = unpack(total, 1) * t * inverse
    a22 = unpack(total, 2) * t * t
    ww = unpack(total, 3) * t * t
    n1 = load_square * inverse * inverse
    n2 = q_square * t * t
    g12 = h11 * EPS * inverse * t
    h22 = a22 - h12 * g12
    left = (
        ww
        - h12 * h12 * (2.0 - n1)
        - h22 * (2.0 * a22 - h22 * n2)
        + 2.0 * h12 * h22 * g12
    )
    h32 = jnp.sqrt(jnp.maximum(left, 0.0) + EPS)
    r1 = jnp.sqrt(h11 * h11 + h21 * h21)
    c1 = h11 / r1
    s1 = h21 / r1
    top = c1 * h12 + s1 * h22
    low = c1 * h22 - s1 * h12
    r2 = jnp.sqrt(low * low + h32 * h32)
    c2 = low / r2
    s2 = h32 / r2
    y2 = -beta * s1 * c2 / r2
    y1 = (beta * c1 - top * y2) / r1
    norm_ref[...] = beta * s1 * s2
    weight1 = y1 * inverse
    weight2 = y2 * t
    for k in range(slots):
        out_ref[k] = weight1 * z1_ref[k] + weight2 * z2_ref[k]

    for d in range(6):
        wait_sent(0, load_send.at[d], load_recv, d)
        wait_sent(1, prec_send.at[d], prec_recv, d)
        wait_sent(2, u1_send.at[d], u1_recv, d)
        wait_sent(3, part_sent(d), u2_recv, d)
    for number in range(2):
        reduce_wait(number, *plane_args, True)
        reduce_wait(number, *line_args, True)


def gather(table, schur_hbm, diag_ref, precond, load, load_out, prec_out, schur_out, diag_out, mask_out, strips, sems):
    nblk, blk, _ = precond.shape
    cols = load.shape[-1]
    slots = table.shape[0]
    cap = slots // 6
    index = [jnp.minimum(table[s], nblk - 1) for s in range(slots)]
    copies = []
    for s in range(slots):
        at = pl.ds(pl.multiple_of(index[s] * blk, blk), blk)
        copies.append(pltpu.make_async_copy(schur_hbm.at[at], strips.at[s], sems.at[s]))
        copies[-1].start()
    eye = lax.broadcasted_iota(jnp.int32, (blk, blk), 0) == lax.broadcasted_iota(
        jnp.int32, (blk, blk), 1
    )
    for s in range(slots):
        d, k = divmod(s, cap)
        valid = table[s] < nblk
        load_out[d, k * blk : (k + 1) * blk] = jnp.where(valid, load[index[s]].astype(F32), 0.0)
        prec_out[d, k] = precond[index[s]]
        mask_out[s] = jnp.full((8, cols), jnp.where(valid, 1.0, 0.0), F32)
        line = diag_ref[:, pl.ds(pl.multiple_of(index[s] * blk, blk), blk)]
        column = jnp.sum(jnp.where(eye, line, 0.0), axis=1, keepdims=True)
        diag_out[s * blk : (s + 1) * blk] = jnp.broadcast_to(column, (blk, LANES))
    for s in range(slots):
        copies[s].wait()
        for t in range(slots):
            at = pl.ds(pl.multiple_of(index[t] * blk, blk), blk)
            schur_out[s * blk : (s + 1) * blk, t * blk : (t + 1) * blk] = strips[s, :, at]


def place(table, compact, out_ref):
    slots = table.shape[0]
    many = out_ref.shape[0]
    first = pl.program_id(0) * many
    for b in range(many):
        found = jnp.int32(slots)
        for s in range(slots):
            found = jnp.where(table[s] == first + b, jnp.int32(s), found)
        value = compact[jnp.minimum(found, slots - 1)]
        out_ref[b] = jnp.where(found < slots, value, 0.0)


def on_device(sizes, schur, interface_diag, precond, load, face_blocks):
    nblk, blk = precond.shape[3:5]
    cols = load.shape[-1]
    order = schur.shape[-1]
    cap = face_blocks.shape[-1]
    slots = 6 * cap
    rows = cap * blk
    nx, ny, nz = sizes
    planes = ny * nz
    packed = -(-(4 * cols // LANES) // 8) * 8
    vmem = pltpu.VMEM
    dma = pltpu.SemaphoreType.DMA
    anywhere = pl.BlockSpec(memory_space=pl.ANY)
    local = pl.BlockSpec(memory_space=pltpu.VMEM)
    scalars = pl.BlockSpec(memory_space=pltpu.SMEM)
    table = face_blocks.reshape(slots)
    mib = 1024 * 1024
    gathered = pl.pallas_call(
        gather,
        out_shape=(
            jax.ShapeDtypeStruct((6, rows, cols), F32),
            jax.ShapeDtypeStruct((6, cap, blk, blk), F32),
            jax.ShapeDtypeStruct((slots * blk, slots * blk), BF16),
            jax.ShapeDtypeStruct((slots * blk, LANES), F32),
            jax.ShapeDtypeStruct((slots, 8, cols), F32),
        ),
        in_specs=[scalars, anywhere, local, local, local],
        out_specs=(local,) * 5,
        scratch_shapes=[vmem((slots, blk, order), BF16), dma((slots,))],
        compiler_params=pltpu.CompilerParams(vmem_limit_bytes=24 * mib),
    )(
        table,
        schur.reshape(order, order),
        interface_diag.reshape(1, order),
        precond.reshape(nblk, blk, blk),
        load.reshape(nblk, blk, cols),
    )
    compact, norm = pl.pallas_call(
        functools.partial(kernel, sizes),
        out_shape=(
            jax.ShapeDtypeStruct((slots, blk, cols), F32),
            jax.ShapeDtypeStruct((1, cols), F32),
        ),
        in_specs=[local] * 5,
        out_specs=(local, local),
        scratch_shapes=[
            vmem((6, rows, cols), F32),
            vmem((6, cap, blk, blk), F32),
            vmem((slots, blk, 2 * blk), BF16),
            vmem((6, rows, cols), F32),
            vmem((slots, blk, cols), F32),
            vmem((slots, blk, cols), F32),
            vmem((slots * blk, cols), BF16),
            vmem((6, rows, cols), F32),
            vmem((6, rows, cols), F32),
            vmem((6, rows, cols), F32),
            vmem((6, rows, cols), F32),
            vmem((6, rows // 2, cols), F32),
            vmem((2, planes, packed, LANES), F32),
            vmem((2, nx, packed, LANES), F32),
            dma((4, 6)),
            dma((4, 6)),
            dma((2, max(planes - 1, 1))),
            dma((2, max(planes - 1, 1))),
            dma((2, max(nx - 1, 1))),
            dma((2, max(nx - 1, 1))),
        ],
        compiler_params=pltpu.CompilerParams(
            collective_id=0, has_side_effects=True, vmem_limit_bytes=32 * mib
        ),
    )(*gathered)
    many = 4 if nblk % 4 == 0 else 1
    result = pl.pallas_call(
        place,
        grid=(nblk // many,),
        out_shape=jax.ShapeDtypeStruct((nblk, blk, cols), F32),
        in_specs=[scalars, local],
        out_specs=pl.BlockSpec((many, blk, cols), lambda i: (i, 0, 0)),
        compiler_params=pltpu.CompilerParams(vmem_limit_bytes=16 * mib),
    )(table, compact)
    return result.reshape(1, 1, 1, nblk * blk, cols), norm.reshape(cols)


def solution(mesh):
    sizes = tuple(mesh.shape[a] for a in AXES)
    placed = (
        P("gx", "gy", "gz", None, None),
        P("gx", "gy", "gz", None),
        P("gx", "gy", "gz", None, None, None),
        P("gx", "gy", "gz", None, None),
        P("gx", "gy", "gz", None, None),
    )
    return jax.shard_map(
        functools.partial(on_device, sizes),
        mesh=mesh,
        in_specs=placed,
        out_specs=(P("gx", "gy", "gz", None, None), P()),
        check_vma=False,
    )
```
